256 devices in a mesh: src: 8 (over x, y_hi), rcv: 32 (over y_lo, z, core).
Axes of the slice: x: 4, y: 4 (y_hi: 2, y_lo: 2; y = y_hi * 2 + y_lo), z: 8, core: 2. Of those that a mesh axis runs over, the one named last changes fastest.
Arguments:
- wavefield: float32 [2, 16, 2048, 2048], P(None, None, 'rcv', 'src')
- surface_band: float32 [2, 2048, 1024], P(None, 'rcv'), may hold values from -0.75 to 0.75
- band_shift: int32 [32], P('rcv'), may hold values from -16 to 16
- trace_mask: int32 [2048], P('rcv'), may hold values 0 or 1
- shot_taper: float32 [5], replicated, may hold values from 0.2 to 1
Outputs:
- multiples: float32 [2, 16, 2048, 2048], P(None, None, 'rcv', 'src')
- primaries: float32 [2, 16, 2048, 2048], P(None, None, 'rcv', 'src')
The draws below stay inside these ranges and needn't reach their ends.
All inputs are finite; a program needn't handle non-finite values. No bound on the sum of `trace_mask` on one device may be relied on, other than what follows from the above.
Results may differ from the reference program's by a relative error of at most 0.0003.
Values sent between devices are 32-bit elements; how exact they have to be, the bound alone decides.
A program may use at most 64 MiB of HBM per device.

```python
import jax
import jax.numpy as jnp
from jax import lax

F = 16
NS = 2048
NR = 2048
APER = 64
SHIFT = 16
BLOCK = 64
SHALF = 2


def draw_wavefield(key, part):
    base_key = jax.random.fold_in(key, 7)
    noise_key, row_key, col_key = jax.random.split(base_key, 3)
    rows = jnp.exp(jax.random.uniform(row_key, (NS,), jnp.float32, -1.15, 1.15)) * jnp.exp(1.0986 * (jnp.arange(NS, dtype=jnp.float32) / NS - 0.5))
    cols = jnp.exp(jax.random.uniform(col_key, (NR,), jnp.float32, -1.15, 1.15)) * jnp.exp(1.0986 * (jnp.arange(NR, dtype=jnp.float32) / NR - 0.5))
    noise = jax.random.normal(noise_key, (2, F, NR, NS), jnp.float32)
    return noise * cols[None, None, :, None] * rows[None, None, None, :] * 0.5


def touch_ends(array, key, least, largest):
    place = [jax.random.randint(jax.random.fold_in(key, axis), (), 0, length) for axis, length in enumerate(array.shape)]
    longest = array.shape.index(max(array.shape))
    neighbour = place[:longest] + [(place[longest] + 1) % array.shape[longest]] + place[longest + 1:]
    return array.at[tuple(place)].set(least).at[tuple(neighbour)].set(largest)


def levels(stream_key, extent, cuts, low, top_value):
    level, own = 1.0, jax.random.fold_in(stream_key, 6)
    for position, shards_of in cuts:
        heights = jnp.exp(jax.random.uniform(jax.random.fold_in(own, position), (shards_of,), jnp.float32, low / len(cuts), top_value / len(cuts)))
        level = level * jnp.repeat(heights, extent[position] // shards_of).reshape([-1 if axis == position else 1 for axis in range(len(extent))])
    return level


def gaussian(stream_key, extent, spread, limit, shards=(), kind=jnp.bfloat16):
    level = levels(stream_key, extent, shards, -0.22, 0.18) if shards else 1.0
    drawn = jax.random.normal(stream_key, extent, jnp.float32) * spread * level
    return jnp.minimum(jnp.maximum(drawn, -limit), limit).astype(kind)


def setup_inputs(seed: int = 0) -> dict:
    key_of = jax.random.split(jax.random.key(seed), 6)
    wavefield = draw_wavefield(jax.random.fold_in(key_of[5], 71), 0)
    surface_band = gaussian(key_of[1], (2, NR, F * APER), APER ** -0.5, 0.75, ((1, 32),), jnp.float32)
    band_shift = touch_ends(jax.random.randint(key_of[2], (NR // BLOCK,), -SHIFT, SHIFT + 1), jax.random.fold_in(key_of[2], 1), -SHIFT, SHIFT).astype(jnp.int32)
    trace_mask = touch_ends((jax.random.randint(key_of[3], (NR,), 0, 8) < 7).astype(jnp.int32), jax.random.fold_in(key_of[3], 1), 0, 1)
    shot_taper = jnp.clip(jax.random.uniform(key_of[4], (2 * SHALF + 1,), jnp.float32, 0.2, 1.0), 0.2, 1.0)
    return dict(wavefield=wavefield, surface_band=surface_band, band_shift=band_shift, trace_mask=trace_mask, shot_taper=shot_taper)


def band_matrix(band_piece):
    columns = band_piece.shape[3]
    taps = band_piece.shape[2]
    rows_index = jnp.arange(columns + taps - 1, dtype=jnp.int32)
    cols_index = jnp.arange(columns, dtype=jnp.int32)
    tap_index = jnp.arange(taps, dtype=jnp.int32)
    onehot = (tap_index[:, None, None] == rows_index[None, :, None] - cols_index[None, None, :]).astype(jnp.float32)
    return jnp.einsum('xftc,tjc->xfjc', band_piece, onehot, precision=lax.Precision.HIGHEST)

def complex_product(window, band):
    real_part = jnp.einsum('fjc,fjs->fcs', band[0], window[0], precision=lax.Precision.HIGHEST) - jnp.einsum('fjc,fjs->fcs', band[1], window[1], precision=lax.Precision.HIGHEST)
    imag_part = jnp.einsum('fjc,fjs->fcs', band[1], window[0], precision=lax.Precision.HIGHEST) + jnp.einsum('fjc,fjs->fcs', band[0], window[1], precision=lax.Precision.HIGHEST)
    return jnp.stack([real_part, imag_part])

def reference(wavefield, surface_band, band_shift, trace_mask, shot_taper):
    masked = wavefield * trace_mask.astype(jnp.float32)[None, None, :, None]
    halo_width = APER // 2 + SHIFT
    padded = jnp.pad(masked, ((0, 0), (0, 0), (halo_width, halo_width), (0, 0)))
    band_full = jnp.transpose(surface_band.reshape(2, NR, F, APER), (0, 2, 3, 1))

    def one_block(index):
        start = index * BLOCK + halo_width - APER // 2 + band_shift[index]
        window = lax.dynamic_slice_in_dim(padded, start.astype(jnp.int32), BLOCK + APER - 1, 2)
        band_piece = lax.dynamic_slice_in_dim(band_full, (index * BLOCK).astype(jnp.int32), BLOCK, 3)
        return complex_product(window, band_matrix(band_piece))
    stacked = lax.map(one_block, jnp.arange(NR // BLOCK, dtype=jnp.int32))
    predicted = jnp.moveaxis(stacked, 0, 2).reshape(2, F, NR, NS)
    shot_padded = jnp.pad(predicted, ((0, 0), (0, 0), (0, 0), (SHALF, SHALF)))
    multiples = jnp.zeros_like(predicted)
    for offset_row in range(2 * SHALF + 1):
        multiples = multiples + shot_taper[offset_row] * shot_padded[:, :, :, offset_row:offset_row + NS]
    data_energy = lax.optimization_barrier(jnp.sum(wavefield * wavefield, axis=(0, 2, 3)))
    pred_energy = lax.optimization_barrier(jnp.sum(multiples * multiples, axis=(0, 2, 3)))
    gain = jnp.sqrt((data_energy + 1e-06) / (pred_energy + 1e-06))
    primaries = wavefield - gain[None, :, None, None] * multiples
    return (multiples, primaries)
```

```python
import functools

import jax
import jax.numpy as jnp
from jax import lax
from jax.experimental import pallas as pl
from jax.experimental.pallas import tpu as pltpu
from jax.sharding import Mesh
from jax.sharding import PartitionSpec as P

APER = 64
LANES = 128
HALO = 48
RCV = ("rcv_0", "rcv_1", "rcv_2")
SRC = ("src_0", "src_1")
NEAR = ("rcv_1", "rcv_2")
FAR = ("src_0", "src_1", "rcv_0")
EARLY = 6
MESH = pl.DeviceIdType.MESH


def place(axes):
    index = 0
    for axis in axes:
        index = index * lax.axis_size(axis) + lax.axis_index(axis)
    return index


def count_of(axes):
    count = 1
    for axis in axes:
        count *= lax.axis_size(axis)
    return count


def at(axes, index):
    coordinates = {}
    for axis in reversed(axes):
        coordinates[axis] = lax.rem(index, lax.axis_size(axis))
        index = index // lax.axis_size(axis)
    return coordinates


def beside(axes, step):
    count = count_of(axes)
    return at(axes, lax.rem(place(axes) + (step + count), count))


def lanes_of(shape):
    return lax.broadcasted_iota(jnp.int32, shape, 1)


def taper(h, x0, x1, weights):
    lane = lanes_of(x0.shape)
    first, last = lane == 0, lane == LANES - 1

    def later(a, b0, b1):
        ra, r0, r1 = (pltpu.roll(v, 1, 1) for v in (a, b0, b1))
        return ra, jnp.where(first, ra, r0), jnp.where(first, r0, r1)

    def sooner(a, b0, b1):
        ra, r0, r1 = (pltpu.roll(v, LANES - 1, 1) for v in (a, b0, b1))
        return ra, jnp.where(last, r1, r0), jnp.where(last, ra, r1)

    parts = (h, x0, x1)
    below = later(*(weights[0] * v for v in parts))
    below = later(*(s + weights[1] * v for s, v in zip(below, parts)))
    above = sooner(*(weights[4] * v for v in parts))
    above = sooner(*(s + weights[3] * v for s, v in zip(above, parts)))
    return tuple(below[i] + weights[2] * parts[i] + above[i] for i in (1, 2))


def halves(value):
    high = value.astype(jnp.bfloat16)
    return high, (value - high.astype(jnp.float32)).astype(jnp.bfloat16)


def kernel(
    x_hbm, band_hbm, shift_ref, mask_hbm, taper_ref,
    mult_ref, prim_ref,
    xv, bandv, mask_own, mask_left, mask_right, edges, edges_left, edges_right,
    rim, rim_left, rim_right, left, right, bands, high, low, row, near, far,
    x_sem, band_sem, mask_sem, send_sem, left_sem, right_sem, aux_send, aux_recv,
    near_send, near_recv, far_send, far_recv,
):
    slices = xv.shape[1]
    groups = x_sem.shape[0]
    per_group = slices // groups
    weights = [taper_ref[i] for i in range(5)]
    shift = shift_ref[0]

    def fetch(g):
        part = pl.ds(g * per_group, per_group)
        return pltpu.make_async_copy(x_hbm.at[:, part], xv.at[:, part], x_sem.at[g])

    for g in range(groups):
        fetch(g).start()
    mask_copy = pltpu.make_async_copy(mask_hbm, mask_own, mask_sem)
    mask_copy.start()
    band_copy = pltpu.make_async_copy(band_hbm, bandv, band_sem)
    band_copy.start()

    before, after = beside(RCV, -1), beside(RCV, 1)
    near_count, far_count = count_of(NEAR), count_of(FAR)
    near_me, far_me = place(NEAR), place(FAR)
    barrier = pltpu.get_barrier_semaphore()
    pl.semaphore_signal(barrier, inc=1, device_id=before, device_id_type=MESH)
    pl.semaphore_signal(barrier, inc=1, device_id=after, device_id_type=MESH)
    for axes, count in ((NEAR, near_count), (FAR, far_count)):
        @pl.loop(1, count)
        def _(step):
            pl.semaphore_signal(barrier, inc=1, device_id=beside(axes, step), device_id_type=MESH)

    for g in range(groups):
        fetch(g).wait()
    mask_copy.wait()

    def pack(p, packed):
        c, f = p // slices, lax.rem(p, slices)
        x0, x1 = xv[c, f, :, :LANES], xv[c, f, :, LANES:]
        lane = lanes_of(x0.shape)
        ends = jnp.where(lane < 2, x0, jnp.where(lane >= LANES - 2, x1, 0.0))
        return packed + pltpu.roll(ends, 4 * p + 2, 1)

    edges[...] = lax.fori_loop(0, 2 * slices, pack, jnp.zeros(edges.shape, jnp.float32))
    pl.semaphore_wait(barrier, 2 + (near_count - 1) + (far_count - 1))

    def to_left(f):
        return pltpu.make_async_remote_copy(
            src_ref=xv.at[:, f, pl.ds(0, HALO)], dst_ref=right.at[f],
            send_sem=send_sem.at[0, f], recv_sem=right_sem.at[f],
            device_id=before, device_id_type=MESH)

    def to_right(f):
        return pltpu.make_async_remote_copy(
            src_ref=xv.at[:, f, pl.ds(BLOCK_ROWS - HALO, HALO)], dst_ref=left.at[f],
            send_sem=send_sem.at[1, f], recv_sem=left_sem.at[f],
            device_id=after, device_id_type=MESH)

    def aux(i, source, target, device):
        return pltpu.make_async_remote_copy(
            src_ref=source, dst_ref=target, send_sem=aux_send.at[i], recv_sem=aux_recv.at[i],
            device_id=device, device_id_type=MESH)

    mask_copies = (aux(0, mask_own, mask_right, before), aux(1, mask_own, mask_left, after))
    edge_copies = (aux(2, edges, edges_right, beside(SRC, -1)), aux(3, edges, edges_left, beside(SRC, 1)))
    rim_copies = (
        aux(4, rim.at[pl.ds(0, HALO)], rim_right, before),
        aux(5, rim.at[pl.ds(BLOCK_ROWS - HALO, HALO)], rim_left, after))
    for copy in mask_copies:
        copy.start()

    @pl.loop(0, EARLY)
    def _(f):
        to_left(f).start()
        to_right(f).start()

    for copy in edge_copies:
        copy.start()

    lane_row = lanes_of((1, LANES))

    def data_part(f, energy):
        x = xv[:, f]
        return jnp.where(lane_row == f, jnp.sum(x * x), energy)

    energy = lax.fori_loop(0, slices, data_part, jnp.zeros((1, LANES), jnp.float32))

    for copy in mask_copies:
        copy.wait_recv()
    place_r, count_r = place(RCV), count_of(RCV)
    has_left = (place_r > 0).astype(jnp.float32)
    has_right = (place_r < count_r - 1).astype(jnp.float32)
    lane_half = lanes_of((1, BLOCK_ROWS))
    m_own = mask_own[...].astype(jnp.float32)
    m_left = mask_left[...].astype(jnp.float32) * has_left
    m_right = mask_right[...].astype(jnp.float32) * has_right
    mask = jnp.concatenate([m_own, jnp.where(lane_half <= 30 + shift, m_right, m_left)], axis=1)

    band_copy.wait()

    @pl.loop(0, slices // 2)
    def _(g):
        lane = lanes_of((BLOCK_ROWS, LANES))
        for odd in range(2):
            f = 2 * g + odd
            pieces = []
            for c in range(2):
                tile = bandv[c, :, pl.ds(pl.multiple_of(g * LANES, LANES), LANES)]
                tile = jnp.where((lane >= APER) if odd else (lane < APER), tile, 0.0)
                turn = shift + (LANES - APER // 2 - odd * APER)
                tile = pltpu.roll(pltpu.roll(tile, turn, 1), 0, 1, stride=1, stride_axis=0)
                pieces.append(halves(tile * mask))
            for k in range(2):
                real, imag = pieces[0][k], pieces[1][k]
                base = 2 * BLOCK_ROWS * k
                bands[f, base:base + BLOCK_ROWS, :LANES] = real
                bands[f, base:base + BLOCK_ROWS, LANES:] = -imag
                bands[f, base + BLOCK_ROWS:base + 2 * BLOCK_ROWS, :LANES] = imag
                bands[f, base + BLOCK_ROWS:base + 2 * BLOCK_ROWS, LANES:] = real

    for copy in edge_copies:
        copy.wait_recv()
    place_s, count_s = place(SRC), count_of(SRC)
    lane = lanes_of(edges.shape)
    from_left = edges_left[...] * (place_s > 0).astype(jnp.float32)
    from_right = edges_right[...] * (place_s < count_s - 1).astype(jnp.float32)
    rim[...] = jnp.where(lax.rem(lane, 4) < 2, from_left, from_right)
    for copy in rim_copies:
        copy.start()

    @pl.loop(EARLY, slices)
    def _(f):
        to_left(f).start()
        to_right(f).start()

    def put(f, c, rows, values):
        for side, value in enumerate(values):
            h, l = halves(value)
            high[f, pl.ds(c * LANES + rows, BLOCK_ROWS), side * LANES:(side + 1) * LANES] = h
            low[f, pl.ds(c * LANES + rows, BLOCK_ROWS), side * LANES:(side + 1) * LANES] = l

    @pl.loop(0, slices)
    def _(f):
        for c in range(2):
            h = pltpu.roll(rim[...], LANES - 2 - 4 * (c * slices + f), 1)
            put(f, c, 0, taper(h, xv[c, f, :, :LANES], xv[c, f, :, LANES:], weights))

    for copy in rim_copies:
        copy.wait_recv()

    def blend(r, l):
        rows = lax.broadcasted_iota(jnp.int32, (32, r.shape[1]), 0) + 16
        return jnp.concatenate([r[:16], jnp.where(rows <= 30 + shift, r[16:], l[:32]), l[32:]], axis=0)

    rim_halo = blend(rim_right[...], rim_left[...])

    def finish(f, energy):
        to_left(f).wait_recv()
        to_right(f).wait_recv()
        for c in range(2):
            h = pltpu.roll(rim_halo, LANES - 2 - 4 * (c * slices + f), 1)
            x = blend(right[f, c], left[f, c])
            put(f, c, BLOCK_ROWS, taper(h, x[:, :LANES], x[:, LANES:], weights))
        wide = jnp.dot(bands[f], high[f], preferred_element_type=jnp.float32)
        thin = jnp.dot(bands[f, :LANES], low[f], preferred_element_type=jnp.float32)
        result = wide[:LANES] + wide[LANES:] + thin
        mult_ref[0, f] = result[:BLOCK_ROWS]
        mult_ref[1, f] = result[BLOCK_ROWS:]
        return jnp.where(lane_row == f + slices, jnp.sum(result * result), energy)

    energy = lax.fori_loop(0, slices, finish, energy)

    def total(axes, me, count, slots, sends, recvs, energy, stage):
        row[stage] = energy
        slots[me] = energy

        def copy(step):
            return pltpu.make_async_remote_copy(
                src_ref=row.at[stage], dst_ref=slots.at[me], send_sem=sends.at[step], recv_sem=recvs.at[me],
                device_id=beside(axes, step), device_id_type=MESH)

        def arrival(step):
            other = lax.rem(me + step, count)
            return pltpu.make_async_remote_copy(
                src_ref=row.at[stage], dst_ref=slots.at[other], send_sem=sends.at[step], recv_sem=recvs.at[other],
                device_id=beside(axes, step), device_id_type=MESH)

        @pl.loop(1, count)
        def _(step):
            copy(step).start()

        @pl.loop(1, count)
        def _(step):
            arrival(step).wait_recv()

        result = slots[0]
        for slot in range(1, count):
            result = result + slots[slot]

        @pl.loop(1, count)
        def _(step):
            copy(step).wait_send()

        return result

    energy = total(NEAR, near_me, near_count, near, near_send, near_recv, energy, 0)
    energy = total(FAR, far_me, far_count, far, far_send, far_recv, energy, 1)
    predicted = pltpu.roll(energy, LANES - slices, 1)
    gain = jnp.sqrt((energy + 1e-06) / (predicted + 1e-06))

    @pl.loop(0, slices)
    def _(f):
        scale = jnp.sum(jnp.where(lane_row == f, gain, 0.0))
        prim_ref[:, f] = xv[:, f] - scale * mult_ref[:, f]

    for copy in mask_copies + edge_copies + rim_copies:
        copy.wait_send()

    @pl.loop(0, slices)
    def _(f):
        to_left(f).wait_send()
        to_right(f).wait_send()


BLOCK_ROWS = 64


def per_device(wavefield, surface_band, band_shift, trace_mask, shot_taper):
    _, slices, receivers, shots = wavefield.shape
    near_count, far_count = count_of(NEAR), count_of(FAR)
    groups = 4
    anywhere = pl.BlockSpec(memory_space=pl.ANY)
    scalars = pl.BlockSpec(memory_space=pltpu.SMEM)
    whole = pl.BlockSpec(memory_space=pltpu.VMEM)
    f32, bf16 = jnp.float32, jnp.bfloat16
    dma = pltpu.SemaphoreType.DMA
    return pl.pallas_call(
        kernel,
        out_shape=(jax.ShapeDtypeStruct(wavefield.shape, f32),) * 2,
        in_specs=[anywhere, anywhere, scalars, anywhere, scalars],
        out_specs=(whole, whole),
        scratch_shapes=[
            pltpu.VMEM(wavefield.shape, f32),
            pltpu.VMEM(surface_band.shape, f32),
            pltpu.VMEM((1, receivers), jnp.int32),
            pltpu.VMEM((1, receivers), jnp.int32),
            pltpu.VMEM((1, receivers), jnp.int32),
            pltpu.VMEM((receivers, LANES), f32),
            pltpu.VMEM((receivers, LANES), f32),
            pltpu.VMEM((receivers, LANES), f32),
            pltpu.VMEM((receivers, LANES), f32),
            pltpu.VMEM((HALO, LANES), f32),
            pltpu.VMEM((HALO, LANES), f32),
            pltpu.VMEM((slices, 2, HALO, shots), f32),
            pltpu.VMEM((slices, 2, HALO, shots), f32),
            pltpu.VMEM((slices, 4 * receivers, 2 * LANES), bf16),
            pltpu.VMEM((slices, 2 * LANES, shots), bf16),
            pltpu.VMEM((slices, 2 * LANES, shots), bf16),
            pltpu.VMEM((2, 1, LANES), f32),
            pltpu.VMEM((near_count, 1, LANES), f32),
            pltpu.VMEM((far_count, 1, LANES), f32),
            dma((groups,)),
            dma(()),
            dma(()),
            dma((2, slices)),
            dma((slices,)),
            dma((slices,)),
            dma((6,)),
            dma((6,)),
            dma((near_count,)),
            dma((near_count,)),
            dma((far_count,)),
            dma((far_count,)),
        ],
        compiler_params=pltpu.CompilerParams(
            collective_id=0, has_side_effects=True, vmem_limit_bytes=48 * 1024 * 1024),
        name="predict",
    )(wavefield, surface_band, band_shift, trace_mask.reshape(1, receivers), shot_taper)


def solution(mesh):
    sizes = SPLIT_SIZES or (4, 2, 2, 8, 2)
    split = Mesh(mesh.devices.reshape(sizes), SRC + RCV)
    return jax.shard_map(
        per_device,
        mesh=split,
        in_specs=(P(None, None, RCV, SRC), P(None, RCV, None), P(RCV), P(RCV), P()),
        out_specs=(P(None, None, RCV, SRC), P(None, None, RCV, SRC)),
        check_vma=False,
    )


SPLIT_SIZES = None
```

```python
import jax
import jax.numpy as jnp
from jax import lax
from jax.experimental import pallas as pl
from jax.experimental.pallas import tpu as pltpu
from jax.sharding import Mesh
from jax.sharding import PartitionSpec as P

APER = 64
LANES = 128
ROWS = 64
HALO = 48
RCV = ("rcv_0", "rcv_1", "rcv_2")
SRC = ("src_0", "src_1")
NEAR = ("rcv_1", "rcv_2")
FAR = ("src_0", "src_1", "rcv_0")
EARLY = 6
EARLY_FAR = 3
GROUPS = 4
MESH = pl.DeviceIdType.MESH
SPLIT_SIZES = (4, 2, 2, 8, 2)


def place(axes):
    index = 0
    for axis in axes:
        index = index * lax.axis_size(axis) + lax.axis_index(axis)
    return index


def count_of(axes):
    count = 1
    for axis in axes:
        count *= lax.axis_size(axis)
    return count


def at(axes, index):
    coordinates = {}
    for axis in reversed(axes):
        coordinates[axis] = lax.rem(index, lax.axis_size(axis))
        index = index // lax.axis_size(axis)
    return coordinates


def beside(axes, step):
    count = count_of(axes)
    return at(axes, lax.rem(place(axes) + (step + count), count))


def lanes_of(shape):
    return lax.broadcasted_iota(jnp.int32, shape, 1)


def rows_of(shape):
    return lax.broadcasted_iota(jnp.int32, shape, 0)


def taper(h, x0, x1, weights):
    lane = lanes_of(x0.shape)
    y0, y1 = weights[2] * x0, weights[2] * x1
    for step in (1, 2):
        wrap = lane >= LANES - step
        y0 += weights[2 - step] * pltpu.roll(jnp.where(wrap, h, x0), step, 1)
        y1 += weights[2 - step] * pltpu.roll(jnp.where(wrap, x0, x1), step, 1)
        wrap = lane < step
        y0 += weights[2 + step] * pltpu.roll(jnp.where(wrap, x1, x0), LANES - step, 1)
        y1 += weights[2 + step] * pltpu.roll(jnp.where(wrap, h, x1), LANES - step, 1)
    return y0, y1


def halves(value):
    high = value.astype(jnp.bfloat16)
    return high, (value - high.astype(jnp.float32)).astype(jnp.bfloat16)


def predict(
    x_hbm, band_hbm, shift_ref, mask_hbm, taper_hbm,
    xv, mult_ref, gain_ref,
    taper_ref, bandv, mask_own, mask_left, mask_right, edges, edges_left, edges_right,
    rim, rim_left, rim_right, left, right, bands, high, low, parts, row, near, far,
    x_sem, band_sem, mask_sem, taper_sem, send_sem, left_sem, right_sem, aux_send, aux_recv,
    near_send, near_recv, far_send, far_recv,
):
    slices = xv.shape[1]
    per_group = slices // GROUPS

    def fetch(g):
        part = pl.ds(g * per_group, per_group)
        return pltpu.make_async_copy(x_hbm.at[:, part], xv.at[:, part], x_sem.at[g])

    for g in range(GROUPS):
        fetch(g).start()
    mask_copy = pltpu.make_async_copy(mask_hbm, mask_own, mask_sem)
    mask_copy.start()
    band_copy = pltpu.make_async_copy(band_hbm, bandv, band_sem)
    band_copy.start()
    taper_copy = pltpu.make_async_copy(taper_hbm, taper_ref, taper_sem)
    taper_copy.start()

    before, after = beside(RCV, -1), beside(RCV, 1)
    has_before, has_after = place(RCV) > 0, place(RCV) < count_of(RCV) - 1
    has_lower, has_upper = place(SRC) > 0, place(SRC) < count_of(SRC) - 1
    near_count, far_count = count_of(NEAR), count_of(FAR)
    near_me, far_me = place(NEAR), place(FAR)
    barrier = pltpu.get_barrier_semaphore()
    for flag, device in ((has_before, before), (has_after, after)):
        @pl.when(flag)
        def _():
            pl.semaphore_signal(barrier, inc=1, device_id=device, device_id_type=MESH)
    for axes, count in ((NEAR, near_count), (FAR, far_count)):
        @pl.loop(1, count)
        def _(step):
            pl.semaphore_signal(barrier, inc=1, device_id=beside(axes, step), device_id_type=MESH)

    def to_left(f):
        return pltpu.make_async_remote_copy(
            src_ref=xv.at[:, f, pl.ds(0, HALO)], dst_ref=right.at[f],
            send_sem=send_sem.at[0, f], recv_sem=right_sem.at[f],
            device_id=before, device_id_type=MESH)

    def to_right(f):
        return pltpu.make_async_remote_copy(
            src_ref=xv.at[:, f, pl.ds(ROWS - HALO, HALO)], dst_ref=left.at[f],
            send_sem=send_sem.at[1, f], recv_sem=left_sem.at[f],
            device_id=after, device_id_type=MESH)

    def aux(i, source, target, device):
        return pltpu.make_async_remote_copy(
            src_ref=source, dst_ref=target, send_sem=aux_send.at[i], recv_sem=aux_recv.at[i],
            device_id=device, device_id_type=MESH)

    masks = ((aux(0, mask_own, mask_right, before), has_before, has_after),
             (aux(1, mask_own, mask_left, after), has_after, has_before))
    ends = ((aux(2, edges, edges_right, beside(SRC, -1)), has_lower, has_upper),
            (aux(3, edges, edges_left, beside(SRC, 1)), has_upper, has_lower))
    rims = ((aux(4, rim.at[pl.ds(0, HALO)], rim_right, before), has_before, has_after),
            (aux(5, rim.at[pl.ds(ROWS - HALO, HALO)], rim_left, after), has_after, has_before))

    def start(entries):
        for copy, sends, _ in entries:
            pl.when(sends)(copy.start)

    def arrive(entries):
        for copy, _, receives in entries:
            pl.when(receives)(copy.wait_recv)

    early_left = jnp.where(near_me == 0, EARLY_FAR, EARLY)
    early_right = jnp.where(near_me == near_count - 1, EARLY_FAR, EARLY)

    def bulk(copy, flag, first, last):
        @pl.when(flag)
        def _():
            @pl.loop(first, last)
            def _(f):
                copy(f).start()

    for g in range(GROUPS):
        fetch(g).wait()
    for copy in (mask_copy, taper_copy):
        copy.wait()
    weights = [taper_ref[i] for i in range(5)]
    shift = shift_ref[0]

    with jax.named_scope("pack"):
        def pack(f, packed):
            for c in range(2):
                x0, x1 = xv[c, f, :, :LANES], xv[c, f, :, LANES:]
                lane = lanes_of(x0.shape)
                tips = jnp.where(lane < 2, x0, jnp.where(lane >= LANES - 2, x1, 0.0))
                packed = packed + pltpu.roll(tips, 4 * (c * slices + f) + 2, 1)
            return packed

        edges[...] = lax.fori_loop(0, slices, pack, jnp.zeros(edges.shape, jnp.float32), unroll=4)

    with jax.named_scope("barrier"):
        neighbours = has_before.astype(jnp.int32) + has_after.astype(jnp.int32)
        pl.semaphore_wait(barrier, neighbours + (near_count - 1) + (far_count - 1))

    start(ends)
    start(masks)
    bulk(to_left, has_before, 0, early_left)
    bulk(to_right, has_after, 0, early_right)

    with jax.named_scope("clear"):
        @pl.when(jnp.logical_not(has_before))
        def _():
            mask_left[...] = jnp.zeros_like(mask_left)
            rim_left[...] = jnp.zeros_like(rim_left)
            left[...] = jnp.zeros_like(left)

        @pl.when(jnp.logical_not(has_after))
        def _():
            mask_right[...] = jnp.zeros_like(mask_right)
            rim_right[...] = jnp.zeros_like(rim_right)
            right[...] = jnp.zeros_like(right)

        @pl.when(jnp.logical_not(has_lower))
        def _():
            edges_left[...] = jnp.zeros_like(edges_left)

        @pl.when(jnp.logical_not(has_upper))
        def _():
            edges_right[...] = jnp.zeros_like(edges_right)

    with jax.named_scope("maskwait"):
        arrive(masks)
    lane_half = lanes_of((1, ROWS))
    m_own, m_left, m_right = (m[...].astype(jnp.float32) for m in (mask_own, mask_left, mask_right))
    mask = jnp.concatenate([m_own, jnp.where(lane_half <= 30 + shift, m_right, m_left)], axis=1)

    band_copy.wait()

    with jax.named_scope("bands"):
        @pl.loop(0, slices // 2)
        def _(g):
            lane = lanes_of((ROWS, LANES))
            for odd in range(2):
                f = 2 * g + odd
                pieces = []
                for c in range(2):
                    tile = bandv[c, :, pl.ds(pl.multiple_of(g * LANES, LANES), LANES)]
                    tile = jnp.where((lane >= APER) if odd else (lane < APER), tile, 0.0)
                    turn = shift + (LANES - APER // 2 - odd * APER)
                    tile = pltpu.roll(pltpu.roll(tile, turn, 1), 0, 1, stride=1, stride_axis=0)
                    pieces.append(halves(tile * mask))
                for k in range(2):
                    real, imag = pieces[0][k], pieces[1][k]
                    base = 2 * ROWS * k
                    bands[f, base:base + ROWS, :LANES] = real
                    bands[f, base:base + ROWS, LANES:] = -imag
                    bands[f, base + ROWS:base + 2 * ROWS, :LANES] = imag
                    bands[f, base + ROWS:base + 2 * ROWS, LANES:] = real

    with jax.named_scope("edgewait"):
        arrive(ends)
    rim[...] = jnp.where(lax.rem(lanes_of(rim.shape), 4) < 2, edges_left[...], edges_right[...])
    start(rims)
    bulk(to_left, has_before, early_left, slices)
    bulk(to_right, has_after, early_right, slices)

    def put(f, c, first, values):
        for side, value in enumerate(values):
            h, l = halves(value)
            columns = slice(side * LANES, (side + 1) * LANES)
            high[f, pl.ds(c * LANES + first, ROWS), columns] = h
            low[f, pl.ds(c * LANES + first, ROWS), columns] = l

    with jax.named_scope("own"):
        @pl.loop(0, slices)
        def _(f):
            squares = jnp.zeros((1, LANES), jnp.float32)
            for c in range(2):
                h = pltpu.roll(rim[...], LANES - 2 - 4 * (c * slices + f), 1)
                x0, x1 = xv[c, f, :, :LANES], xv[c, f, :, LANES:]
                put(f, c, 0, taper(h, x0, x1, weights))
                squares += jnp.sum(x0 * x0 + x1 * x1, axis=0, keepdims=True)
            parts[pl.ds(f, 1), :] = squares

    with jax.named_scope("rimwait"):
        arrive(rims)

    def blend(r, l):
        rows = rows_of((32, r.shape[1])) + 16
        return jnp.concatenate([r[:16], jnp.where(rows <= 30 + shift, r[16:], l[:32]), l[32:]], axis=0)

    rim_halo = blend(rim_right[...], rim_left[...])

    @pl.loop(0, slices)
    def _(f):
        with jax.named_scope("bulkwait"):
            pl.when(has_after)(to_left(f).wait_recv)
            pl.when(has_before)(to_right(f).wait_recv)
        for c in range(2):
            h = pltpu.roll(rim_halo, LANES - 2 - 4 * (c * slices + f), 1)
            x = blend(right[f, c], left[f, c])
            put(f, c, ROWS, taper(h, x[:, :LANES], x[:, LANES:], weights))
        wide = jnp.dot(bands[f], high[f], preferred_element_type=jnp.float32)
        thin = jnp.dot(bands[f, :LANES], low[f], preferred_element_type=jnp.float32)
        result = wide[:LANES] + wide[LANES:] + thin
        mult_ref[0, f] = result[:ROWS]
        mult_ref[1, f] = result[ROWS:]
        squares = jnp.sum(result * result, axis=0, keepdims=True)
        parts[pl.ds(slices + f, 1), :] = squares[:, :LANES] + squares[:, LANES:]

    shape = parts.shape
    diagonal = lanes_of(shape) == rows_of(shape)

    def to_row(column):
        return jnp.sum(jnp.where(diagonal, column, 0.0), axis=0, keepdims=True)

    def total(axes, me, count, slots, sends, recvs, energy, stage):
        row[stage] = energy
        slots[me] = energy

        def copy(step, slot):
            return pltpu.make_async_remote_copy(
                src_ref=row.at[stage], dst_ref=slots.at[slot], send_sem=sends.at[step], recv_sem=recvs.at[slot],
                device_id=beside(axes, step), device_id_type=MESH)

        @pl.loop(1, count)
        def _(step):
            copy(step, me).start()

        @pl.loop(1, count)
        def _(step):
            copy(step, lax.rem(me + step, count)).wait_recv()

        result = slots[0]
        for slot in range(1, count):
            result = result + slots[slot]
        return result

    energy = to_row(jnp.sum(parts[...], axis=1, keepdims=True))
    with jax.named_scope("near"):
        energy = total(NEAR, near_me, near_count, near, near_send, near_recv, energy, 0)
    with jax.named_scope("far"):
        energy = total(FAR, far_me, far_count, far, far_send, far_recv, energy, 1)
    predicted = pltpu.roll(energy, LANES - slices, 1)
    gain = jnp.sqrt((energy + 1e-06) / (predicted + 1e-06))
    spread = jnp.sum(jnp.where(diagonal[:slices], gain, 0.0), axis=1, keepdims=True)
    gain_ref[...] = jnp.broadcast_to(spread, gain_ref.shape)

    with jax.named_scope("sendwait"):
        for copy, sends, _ in masks + ends + rims:
            pl.when(sends)(copy.wait_send)

        @pl.when(has_before)
        def _():
            @pl.loop(0, slices)
            def _(f):
                to_left(f).wait_send()

        @pl.when(has_after)
        def _():
            @pl.loop(0, slices)
            def _(f):
                to_right(f).wait_send()

        for stage, (axes, count, sends) in enumerate(((NEAR, near_count, near_send), (FAR, far_count, far_send))):
            @pl.loop(1, count)
            def _(step):
                pltpu.make_async_remote_copy(
                    src_ref=row.at[stage], dst_ref=row.at[stage], send_sem=sends.at[step], recv_sem=sends.at[step],
                    device_id=beside(axes, step), device_id_type=MESH).wait_send()


def subtract(x_ref, mult_ref, gain_ref, mult_hbm, prim_hbm, prim, mult_sem, prim_sem):
    slices = prim.shape[1]
    per_group = slices // GROUPS

    def copy(source, target, sem, g):
        part = pl.ds(g * per_group, per_group)
        return pltpu.make_async_copy(source.at[:, part], target.at[:, part], sem.at[g])

    for g in range(GROUPS):
        copy(mult_ref, mult_hbm, mult_sem, g).start()
    for g in range(GROUPS):
        @pl.loop(g * per_group, (g + 1) * per_group)
        def _(f):
            scale = gain_ref[pl.ds(f, 1), :]
            for side in range(2):
                columns = slice(side * LANES, (side + 1) * LANES)
                for c in range(2):
                    prim[c, f, :, columns] = x_ref[c, f, :, columns] - scale * mult_ref[c, f, :, columns]

        copy(prim, prim_hbm, prim_sem, g).start()
    for g in range(GROUPS):
        copy(mult_ref, mult_hbm, mult_sem, g).wait()
        copy(prim, prim_hbm, prim_sem, g).wait()


def per_device(wavefield, surface_band, band_shift, trace_mask, shot_taper):
    _, slices, receivers, shots = wavefield.shape
    near_count, far_count = count_of(NEAR), count_of(FAR)
    hbm = pl.BlockSpec(memory_space=pltpu.HBM)
    scalars = pl.BlockSpec(memory_space=pltpu.SMEM)
    whole = pl.BlockSpec(memory_space=pltpu.VMEM)
    f32, bf16 = jnp.float32, jnp.bfloat16
    dma = pltpu.SemaphoreType.DMA
    field = jax.ShapeDtypeStruct(wavefield.shape, f32)
    wavefield, surface_band, trace_mask, shot_taper = (
        pltpu.with_memory_space_constraint(a, pltpu.HBM)
        for a in (wavefield, surface_band, trace_mask.reshape(1, receivers), shot_taper))
    held, multiples, gain = pl.pallas_call(
        predict,
        out_shape=(field, field, jax.ShapeDtypeStruct((slices, LANES), f32)),
        in_specs=[hbm, hbm, scalars, hbm, hbm],
        out_specs=(whole, whole, whole),
        scratch_shapes=[
            pltpu.SMEM(shot_taper.shape, f32),
            pltpu.VMEM(surface_band.shape, f32),
            pltpu.VMEM((1, receivers), jnp.int32),
            pltpu.VMEM((1, receivers), jnp.int32),
            pltpu.VMEM((1, receivers), jnp.int32),
            pltpu.VMEM((receivers, LANES), f32),
            pltpu.VMEM((receivers, LANES), f32),
            pltpu.VMEM((receivers, LANES), f32),
            pltpu.VMEM((receivers, LANES), f32),
            pltpu.VMEM((HALO, LANES), f32),
            pltpu.VMEM((HALO, LANES), f32),
            pltpu.VMEM((slices, 2, HALO, shots), f32),
            pltpu.VMEM((slices, 2, HALO, shots), f32),
            pltpu.VMEM((slices, 4 * receivers, 2 * LANES), bf16),
            pltpu.VMEM((slices, 2 * LANES, shots), bf16),
            pltpu.VMEM((slices, 2 * LANES, shots), bf16),
            pltpu.VMEM((2 * slices, LANES), f32),
            pltpu.VMEM((2, 1, LANES), f32),
            pltpu.VMEM((near_count, 1, LANES), f32),
            pltpu.VMEM((far_count, 1, LANES), f32),
            dma((GROUPS,)),
            dma(()),
            dma(()),
            dma(()),
            dma((2, slices)),
            dma((slices,)),
            dma((slices,)),
            dma((6,)),
            dma((6,)),
            dma((near_count,)),
            dma((near_count,)),
            dma((far_count,)),
            dma((far_count,)),
        ],
        compiler_params=pltpu.CompilerParams(
            collective_id=0, has_side_effects=True, vmem_limit_bytes=40 * 1024 * 1024),
        name="predict",
    )(wavefield, surface_band, band_shift, trace_mask, shot_taper)
    return pl.pallas_call(
        subtract,
        out_shape=(field, field),
        in_specs=[whole, whole, whole],
        out_specs=(hbm, hbm),
        scratch_shapes=[pltpu.VMEM(wavefield.shape, f32), dma((GROUPS,)), dma((GROUPS,))],
        compiler_params=pltpu.CompilerParams(vmem_limit_bytes=16 * 1024 * 1024),
        name="subtract",
    )(held, multiples, gain)


def solution(mesh):
    split = Mesh(mesh.devices.reshape(SPLIT_SIZES), SRC + RCV)
    return jax.shard_map(
        per_device,
        mesh=split,
        in_specs=(P(None, None, RCV, SRC), P(None, RCV, None), P(RCV), P(RCV), P()),
        out_specs=(P(None, None, RCV, SRC), P(None, None, RCV, SRC)),
        check_vma=False,
    )
```

```python
import jax
import jax.numpy as jnp
from jax import lax
from jax.experimental import pallas as pl
from jax.experimental.pallas import tpu as pltpu
from jax.sharding import Mesh
from jax.sharding import PartitionSpec as P

APER = 64
LANES = 128
ROWS = 64
HALO = 48
RCV = ("rcv_0", "rcv_1", "rcv_2")
SRC = ("src_0", "src_1")
NEAR = ("rcv_1", "rcv_2")
FAR = ("src_0", "src_1", "rcv_0")
RINGS = (("src_0",), ("src_1", "rcv_0"), ("rcv_1",), ("rcv_2",))
EARLY = 7
EARLY_FAR = 3
GROUPS = 4
MESH = pl.DeviceIdType.MESH
SPLIT_SIZES = (4, 2, 2, 8, 2)


def place(axes):
    index = 0
    for axis in axes:
        index = index * lax.axis_size(axis) + lax.axis_index(axis)
    return index


def count_of(axes):
    count = 1
    for axis in axes:
        count *= lax.axis_size(axis)
    return count


def at(axes, index):
    coordinates = {}
    for axis in reversed(axes):
        coordinates[axis] = lax.rem(index, lax.axis_size(axis))
        index = index // lax.axis_size(axis)
    return coordinates


def beside(axes, step):
    count = count_of(axes)
    return at(axes, lax.rem(place(axes) + (step + count), count))


def others_of(rings):
    first, second = (count_of(ring) for ring in rings)
    steps = [(i, j) for i in range(first) for j in range(second) if i or j]
    steps.sort(key=lambda step: -min(step[0], first - step[0]) - min(step[1], second - step[1]))
    return [{**beside(rings[0], i), **beside(rings[1], j)} for i, j in steps]


def lanes_of(shape):
    return lax.broadcasted_iota(jnp.int32, shape, 1)


def rows_of(shape):
    return lax.broadcasted_iota(jnp.int32, shape, 0)


def taper(h, x0, x1, weights):
    lane = lanes_of(x0.shape)
    y0, y1 = weights[2] * x0, weights[2] * x1
    for step in (1, 2):
        wrap = lane >= LANES - step
        y0 += weights[2 - step] * pltpu.roll(jnp.where(wrap, h, x0), step, 1)
        y1 += weights[2 - step] * pltpu.roll(jnp.where(wrap, x0, x1), step, 1)
        wrap = lane < step
        y0 += weights[2 + step] * pltpu.roll(jnp.where(wrap, x1, x0), LANES - step, 1)
        y1 += weights[2 + step] * pltpu.roll(jnp.where(wrap, h, x1), LANES - step, 1)
    return y0, y1


def halves(value):
    high = value.astype(jnp.bfloat16)
    return high, (value - high.astype(jnp.float32)).astype(jnp.bfloat16)


def predict(
    x_hbm, band_hbm, shift_ref, mask_hbm, taper_hbm,
    xv, mult_ref, gain_ref,
    taper_ref, bandv, mask_own, mask_left, mask_right, edges, edges_left, edges_right,
    rim, rim_left, rim_right, left, right, bands, high, low, parts, row, near, far,
    x_sem, band_sem, mask_sem, taper_sem, send_sem, left_sem, right_sem, aux_send, aux_recv,
    near_sem, far_sem, known,
):
    slices = xv.shape[1]

    def fetch(i, first, last):
        part = pl.ds(first, last - first)
        return pltpu.make_async_copy(x_hbm.at[:, part], xv.at[:, part], x_sem.at[i])

    fetches = fetch(0, 0, slices // 2), fetch(1, slices // 2, slices)
    for copy in fetches:
        copy.start()
    mask_copy = pltpu.make_async_copy(mask_hbm, mask_own, mask_sem)
    mask_copy.start()
    band_copy = pltpu.make_async_copy(band_hbm, bandv, band_sem)
    band_copy.start()
    taper_copy = pltpu.make_async_copy(taper_hbm, taper_ref, taper_sem)
    taper_copy.start()

    before, after = beside(RCV, -1), beside(RCV, 1)
    lower, upper = beside(SRC, -1), beside(SRC, 1)
    has_before, has_after = place(RCV) > 0, place(RCV) < count_of(RCV) - 1
    has_lower, has_upper = place(SRC) > 0, place(SRC) < count_of(SRC) - 1
    near_count, far_count = count_of(NEAR), count_of(FAR)
    near_me, far_me = place(NEAR), place(FAR)
    def tell(semaphore, device):
        pl.semaphore_signal(semaphore, inc=1, device_id=device, device_id_type=MESH)

    barrier = pltpu.get_barrier_semaphore()
    greeted = sum(flag.astype(jnp.int32) for flag in (has_before, has_after, has_lower, has_upper))
    pl.when(has_lower)(lambda: tell(barrier, lower))
    pl.when(has_upper)(lambda: tell(barrier, upper))
    pl.when(has_before)(lambda: tell(barrier, before))
    pl.when(has_after)(lambda: tell(barrier, after))
    for ring in RINGS:
        if count_of(ring) > 1:
            tell(barrier, beside(ring, -1))
            tell(barrier, beside(ring, 1))
            greeted += 2

    def spread_word(turn):
        for ring in RINGS[:3]:
            if count_of(ring) > 1:
                step = 2 if turn and ring == RINGS[2] and count_of(ring) > 4 else 1
                tell(known.at[turn], beside(ring, -step))
                tell(known.at[turn], beside(ring, step))

    def hear_word(turn):
        pl.semaphore_wait(known.at[turn], 2 * sum(count_of(ring) > 1 for ring in RINGS[:3]))

    def to_left(f):
        return pltpu.make_async_remote_copy(
            src_ref=xv.at[:, f, pl.ds(0, HALO)], dst_ref=right.at[f],
            send_sem=send_sem.at[0], recv_sem=right_sem.at[f],
            device_id=before, device_id_type=MESH)

    def to_right(f):
        return pltpu.make_async_remote_copy(
            src_ref=xv.at[:, f, pl.ds(ROWS - HALO, HALO)], dst_ref=left.at[f],
            send_sem=send_sem.at[1], recv_sem=left_sem.at[f],
            device_id=after, device_id_type=MESH)

    def aux(i, source, target, device):
        return pltpu.make_async_remote_copy(
            src_ref=source, dst_ref=target, send_sem=aux_send.at[i], recv_sem=aux_recv.at[i],
            device_id=device, device_id_type=MESH)

    masks = ((aux(0, mask_own, mask_right, before), has_before, has_after),
             (aux(1, mask_own, mask_left, after), has_after, has_before))
    ends = ((aux(2, edges, edges_right, lower), has_lower, has_upper),
            (aux(3, edges, edges_left, upper), has_upper, has_lower))
    rims = ((aux(4, rim.at[pl.ds(0, HALO)], rim_right, before), has_before, has_after),
            (aux(5, rim.at[pl.ds(ROWS - HALO, HALO)], rim_left, after), has_after, has_before))

    def start(entries):
        for copy, sends, _ in entries:
            pl.when(sends)(copy.start)

    def arrive(entries):
        for copy, _, receives in entries:
            pl.when(receives)(copy.wait_recv)

    early_left = jnp.where(near_me == 0, EARLY_FAR, EARLY)
    early_right = jnp.where(near_me == near_count - 1, EARLY_FAR, EARLY)

    def bulk(copy, flag, first, last):
        @pl.when(flag)
        def _():
            @pl.loop(first, last)
            def _(f):
                copy(f).start()

    for copy in (*fetches, mask_copy, taper_copy):
        copy.wait()
    weights = [taper_ref[i] for i in range(5)]
    shift = shift_ref[0]

    with jax.named_scope("pack"):
        def pack(f, packed):
            for c in range(2):
                x0, x1 = xv[c, f, :, :LANES], xv[c, f, :, LANES:]
                lane = lanes_of(x0.shape)
                tips = jnp.where(lane < 2, x0, jnp.where(lane >= LANES - 2, x1, 0.0))
                packed = packed + pltpu.roll(tips, 4 * (c * slices + f) + 2, 1)
            return packed

        edges[...] = lax.fori_loop(0, slices, pack, jnp.zeros(edges.shape, jnp.float32), unroll=4)

    with jax.named_scope("barrier"):
        pl.semaphore_wait(barrier, greeted)
    start(ends)
    start(masks)
    bulk(to_left, has_before, 0, early_left)
    bulk(to_right, has_after, 0, early_right)
    spread_word(0)

    with jax.named_scope("clear"):
        @pl.when(jnp.logical_not(has_before))
        def _():
            mask_left[...] = jnp.zeros_like(mask_left)
            rim_left[...] = jnp.zeros_like(rim_left)
            left[...] = jnp.zeros_like(left)

        @pl.when(jnp.logical_not(has_after))
        def _():
            mask_right[...] = jnp.zeros_like(mask_right)
            rim_right[...] = jnp.zeros_like(rim_right)
            right[...] = jnp.zeros_like(right)

        @pl.when(jnp.logical_not(has_lower))
        def _():
            edges_left[...] = jnp.zeros_like(edges_left)

        @pl.when(jnp.logical_not(has_upper))
        def _():
            edges_right[...] = jnp.zeros_like(edges_right)

    with jax.named_scope("word0"):
        hear_word(0)
        spread_word(1)
    with jax.named_scope("maskwait"):
        arrive(masks)
    lane_half = lanes_of((1, ROWS))
    m_own, m_left, m_right = (m[...].astype(jnp.float32) for m in (mask_own, mask_left, mask_right))
    mask = jnp.concatenate([m_own, jnp.where(lane_half <= 30 + shift, m_right, m_left)], axis=1)

    band_copy.wait()

    with jax.named_scope("bands"):
        @pl.loop(0, slices // 2)
        def _(g):
            lane = lanes_of((ROWS, LANES))
            for odd in range(2):
                f = 2 * g + odd
                pieces = []
                for c in range(2):
                    tile = bandv[c, :, pl.ds(pl.multiple_of(g * LANES, LANES), LANES)]
                    tile = jnp.where((lane >= APER) if odd else (lane < APER), tile, 0.0)
                    turn = shift + (LANES - APER // 2 - odd * APER)
                    tile = pltpu.roll(pltpu.roll(tile, turn, 1), 0, 1, stride=1, stride_axis=0)
                    pieces.append(halves(tile * mask))
                for k in range(2):
                    real, imag = pieces[0][k], pieces[1][k]
                    base = 2 * ROWS * k
                    bands[f, base:base + ROWS, :LANES] = real
                    bands[f, base:base + ROWS, LANES:] = -imag
                    bands[f, base + ROWS:base + 2 * ROWS, :LANES] = imag
                    bands[f, base + ROWS:base + 2 * ROWS, LANES:] = real

    with jax.named_scope("word1"):
        hear_word(1)
        spread_word(2)
    with jax.named_scope("edgewait"):
        arrive(ends)
    rim[...] = jnp.where(lax.rem(lanes_of(rim.shape), 4) < 2, edges_left[...], edges_right[...])
    start(rims)
    bulk(to_left, has_before, early_left, slices)
    bulk(to_right, has_after, early_right, slices)

    def put(f, c, first, values):
        for side, value in enumerate(values):
            h, l = halves(value)
            columns = slice(side * LANES, (side + 1) * LANES)
            high[f, pl.ds(c * LANES + first, ROWS), columns] = h
            low[f, pl.ds(c * LANES + first, ROWS), columns] = l

    with jax.named_scope("own"):
        @pl.loop(0, slices, unroll=2)
        def _(f):
            squares = jnp.zeros((1, LANES), jnp.float32)
            for c in range(2):
                h = pltpu.roll(rim[...], LANES - 2 - 4 * (c * slices + f), 1)
                x0, x1 = xv[c, f, :, :LANES], xv[c, f, :, LANES:]
                put(f, c, 0, taper(h, x0, x1, weights))
                squares += jnp.sum(x0 * x0 + x1 * x1, axis=0, keepdims=True)
            parts[pl.ds(f, 1), :] = squares

    with jax.named_scope("word2"):
        hear_word(2)
    with jax.named_scope("rimwait"):
        arrive(rims)

    def blend(r, l):
        rows = rows_of((32, r.shape[1])) + 16
        return jnp.concatenate([r[:16], jnp.where(rows <= 30 + shift, r[16:], l[:32]), l[32:]], axis=0)

    rim_halo = blend(rim_right[...], rim_left[...])

    def arrived(f):
        with jax.named_scope("bulkwait"):
            pl.when(has_after)(to_left(f).wait_recv)
            pl.when(has_before)(to_right(f).wait_recv)

    def finish(f):
        for c in range(2):
            h = pltpu.roll(rim_halo, LANES - 2 - 4 * (c * slices + f), 1)
            x = blend(right[f, c], left[f, c])
            put(f, c, ROWS, taper(h, x[:, :LANES], x[:, LANES:], weights))
        wide = jnp.dot(bands[f], high[f], preferred_element_type=jnp.float32)
        thin = jnp.dot(bands[f, :LANES], low[f], preferred_element_type=jnp.float32)
        result = wide[:LANES] + wide[LANES:] + thin
        mult_ref[0, f] = result[:ROWS]
        mult_ref[1, f] = result[ROWS:]
        squares = jnp.sum(result * result, axis=0, keepdims=True)
        parts[pl.ds(slices + f, 1), :] = squares[:, :LANES] + squares[:, LANES:]

    @pl.loop(0, slices // 2 - 1)
    def _(g):
        for f in (2 * g, 2 * g + 1):
            arrived(f)
        for f in (2 * g, 2 * g + 1):
            finish(f)

    @pl.loop(slices - 2, slices)
    def _(f):
        arrived(f)
        finish(f)

    shape = parts.shape
    diagonal = lanes_of(shape) == rows_of(shape)

    def to_row(column):
        return jnp.sum(jnp.where(diagonal, column, 0.0), axis=0, keepdims=True)

    def total(rings, me, count, slots, sems, energy, stage, between):
        row[stage] = energy
        slots[me] = energy

        for device in others_of(rings):
            pltpu.make_async_remote_copy(
                src_ref=row.at[stage], dst_ref=slots.at[me], send_sem=sems.at[0], recv_sem=sems.at[1],
                device_id=device, device_id_type=MESH).start()

        between()
        others = slots.at[pl.ds(0, count - 1)]
        every = pltpu.make_async_remote_copy(
            src_ref=others, dst_ref=others, send_sem=sems.at[0], recv_sem=sems.at[1],
            device_id=beside(rings[0], 1), device_id_type=MESH)
        every.wait_recv()
        result = slots[0]
        for slot in range(1, count):
            result = result + slots[slot]
        return result, every

    def sent():
        for copy, sends, _ in masks + ends + rims:
            pl.when(sends)(copy.wait_send)
        for side, flag, device in ((0, has_before, before), (1, has_after, after)):
            @pl.when(flag)
            def _():
                whole = xv.at[:, :, pl.ds(side * (ROWS - HALO), HALO)]
                pltpu.make_async_remote_copy(
                    src_ref=whole, dst_ref=whole, send_sem=send_sem.at[side], recv_sem=send_sem.at[side],
                    device_id=device, device_id_type=MESH).wait_send()

    energy = to_row(jnp.sum(parts[...], axis=1, keepdims=True))
    with jax.named_scope("near"):
        energy, near_all = total(RINGS[2:], near_me, near_count, near, near_sem, energy, 0, sent)
    with jax.named_scope("far"):
        energy, far_all = total(RINGS[:2], far_me, far_count, far, far_sem, energy, 1, near_all.wait_send)
    predicted = pltpu.roll(energy, LANES - slices, 1)
    gain = jnp.sqrt((energy + 1e-06) / (predicted + 1e-06))
    spread = jnp.sum(jnp.where(diagonal[:slices], gain, 0.0), axis=1, keepdims=True)
    gain_ref[...] = jnp.broadcast_to(spread, gain_ref.shape)

    with jax.named_scope("sendwait"):
        far_all.wait_send()


def subtract(x_ref, mult_ref, gain_ref, mult_hbm, prim_hbm, prim, mult_sem, prim_sem):
    slices = prim.shape[1]
    per_group = slices // GROUPS

    def copy(source, target, sem, g):
        part = pl.ds(g * per_group, per_group)
        return pltpu.make_async_copy(source.at[:, part], target.at[:, part], sem.at[g])

    for g in range(GROUPS):
        copy(mult_ref, mult_hbm, mult_sem, g).start()
    for g in range(GROUPS):
        @pl.loop(g * per_group, (g + 1) * per_group)
        def _(f):
            scale = gain_ref[pl.ds(f, 1), :]
            for side in range(2):
                columns = slice(side * LANES, (side + 1) * LANES)
                for c in range(2):
                    prim[c, f, :, columns] = x_ref[c, f, :, columns] - scale * mult_ref[c, f, :, columns]

        copy(prim, prim_hbm, prim_sem, g).start()
    for g in range(GROUPS):
        copy(mult_ref, mult_hbm, mult_sem, g).wait()
        copy(prim, prim_hbm, prim_sem, g).wait()


def per_device(wavefield, surface_band, band_shift, trace_mask, shot_taper):
    _, slices, receivers, shots = wavefield.shape
    near_count, far_count = count_of(NEAR), count_of(FAR)
    hbm = pl.BlockSpec(memory_space=pltpu.HBM)
    scalars = pl.BlockSpec(memory_space=pltpu.SMEM)
    whole = pl.BlockSpec(memory_space=pltpu.VMEM)
    f32, bf16 = jnp.float32, jnp.bfloat16
    dma = pltpu.SemaphoreType.DMA
    field = jax.ShapeDtypeStruct(wavefield.shape, f32)
    wavefield, surface_band, trace_mask, shot_taper = (
        pltpu.with_memory_space_constraint(a, pltpu.HBM)
        for a in (wavefield, surface_band, trace_mask.reshape(1, receivers), shot_taper))
    held, multiples, gain = pl.pallas_call(
        predict,
        out_shape=(field, field, jax.ShapeDtypeStruct((slices, LANES), f32)),
        in_specs=[hbm, hbm, scalars, hbm, hbm],
        out_specs=(whole, whole, whole),
        scratch_shapes=[
            pltpu.SMEM(shot_taper.shape, f32),
            pltpu.VMEM(surface_band.shape, f32),
            pltpu.VMEM((1, receivers), jnp.int32),
            pltpu.VMEM((1, receivers), jnp.int32),
            pltpu.VMEM((1, receivers), jnp.int32),
            pltpu.VMEM((receivers, LANES), f32),
            pltpu.VMEM((receivers, LANES), f32),
            pltpu.VMEM((receivers, LANES), f32),
            pltpu.VMEM((receivers, LANES), f32),
            pltpu.VMEM((HALO, LANES), f32),
            pltpu.VMEM((HALO, LANES), f32),
            pltpu.VMEM((slices, 2, HALO, shots), f32),
            pltpu.VMEM((slices, 2, HALO, shots), f32),
            pltpu.VMEM((slices, 4 * receivers, 2 * LANES), bf16),
            pltpu.VMEM((slices, 2 * LANES, shots), bf16),
            pltpu.VMEM((slices, 2 * LANES, shots), bf16),
            pltpu.VMEM((2 * slices, LANES), f32),
            pltpu.VMEM((2, 1, LANES), f32),
            pltpu.VMEM((near_count, 1, LANES), f32),
            pltpu.VMEM((far_count, 1, LANES), f32),
            dma((2,)),
            dma(()),
            dma(()),
            dma(()),
            dma((2,)),
            dma((slices,)),
            dma((slices,)),
            dma((6,)),
            dma((6,)),
            dma((2,)),
            dma((2,)),
            pltpu.SemaphoreType.REGULAR((3,)),
        ],
        compiler_params=pltpu.CompilerParams(
            collective_id=0, has_side_effects=True, vmem_limit_bytes=40 * 1024 * 1024),
        name="predict",
    )(wavefield, surface_band, band_shift, trace_mask, shot_taper)
    return pl.pallas_call(
        subtract,
        out_shape=(field, field),
        in_specs=[whole, whole, whole],
        out_specs=(hbm, hbm),
        scratch_shapes=[pltpu.VMEM(wavefield.shape, f32), dma((GROUPS,)), dma((GROUPS,))],
        compiler_params=pltpu.CompilerParams(vmem_limit_bytes=16 * 1024 * 1024),
        name="subtract",
    )(held, multiples, gain)


def solution(mesh):
    split = Mesh(mesh.devices.reshape(SPLIT_SIZES), SRC + RCV)
    return jax.shard_map(
        per_device,
        mesh=split,
        in_specs=(P(None, None, RCV, SRC), P(None, RCV, None), P(RCV), P(RCV), P()),
        out_specs=(P(None, None, RCV, SRC), P(None, None, RCV, SRC)),
        check_vma=False,
    )
```

```python
import jax
import jax.numpy as jnp
from jax import lax
from jax.experimental import pallas as pl
from jax.experimental.pallas import tpu as pltpu
from jax.sharding import Mesh
from jax.sharding import PartitionSpec as P

APER = 64
LANES = 128
ROWS = 64
HALO = 48
RCV = ("rcv_0", "rcv_1", "rcv_2")
SRC = ("src_0", "src_1")
NEAR = ("rcv_1", "rcv_2")
FAR = ("src_0", "src_1", "rcv_0")
RINGS = (("src_0",), ("src_1", "rcv_0"), ("rcv_1",), ("rcv_2",))
EARLY = 6
EARLY_FAR = 2
RELAYED = 5
GROUPS = 4
MESH = pl.DeviceIdType.MESH
SPLIT_SIZES = (4, 2, 2, 8, 2)


def place(axes):
    index = 0
    for axis in axes:
        index = index * lax.axis_size(axis) + lax.axis_index(axis)
    return index


def count_of(axes):
    count = 1
    for axis in axes:
        count *= lax.axis_size(axis)
    return count


def at(axes, index):
    coordinates = {}
    for axis in reversed(axes):
        coordinates[axis] = lax.rem(index, lax.axis_size(axis))
        index = index // lax.axis_size(axis)
    return coordinates


def beside(axes, step):
    count = count_of(axes)
    return at(axes, lax.rem(place(axes) + (step + count), count))


def others_of(rings):
    first, second = (count_of(ring) for ring in rings)
    steps = [(i, j) for i in range(first) for j in range(second) if i or j]
    steps.sort(key=lambda step: -min(step[0], first - step[0]) - min(step[1], second - step[1]))
    return [{**beside(rings[0], i), **beside(rings[1], j)} for i, j in steps]


def lanes_of(shape):
    return lax.broadcasted_iota(jnp.int32, shape, 1)


def rows_of(shape):
    return lax.broadcasted_iota(jnp.int32, shape, 0)


def taper(h, x0, x1, weights):
    lane = lanes_of(x0.shape)
    y0, y1 = weights[2] * x0, weights[2] * x1
    for step in (1, 2):
        wrap = lane >= LANES - step
        y0 += weights[2 - step] * pltpu.roll(jnp.where(wrap, h, x0), step, 1)
        y1 += weights[2 - step] * pltpu.roll(jnp.where(wrap, x0, x1), step, 1)
        wrap = lane < step
        y0 += weights[2 + step] * pltpu.roll(jnp.where(wrap, x1, x0), LANES - step, 1)
        y1 += weights[2 + step] * pltpu.roll(jnp.where(wrap, h, x1), LANES - step, 1)
    return y0, y1


def halves(value):
    high = value.astype(jnp.bfloat16)
    return high, (value - high.astype(jnp.float32)).astype(jnp.bfloat16)


def predict(
    x_hbm, band_hbm, shift_ref, mask_hbm, taper_hbm,
    xv, mult_ref, gain_ref,
    taper_ref, bandv, mask_own, mask_left, mask_right, edges, edges_left, edges_right,
    rim, rim_left, rim_right, left, right, bands, high, low, tips_high, tips_low, fringe, parts, row, near, far,
    x_sem, band_sem, mask_sem, taper_sem, send_sem, left_sem, right_sem, aux_send, aux_recv,
    near_sem, far_sem, known,
):
    slices = xv.shape[1]

    def fetch(i, first, last):
        part = pl.ds(first, last - first)
        return pltpu.make_async_copy(x_hbm.at[:, part], xv.at[:, part], x_sem.at[i])

    fetches = fetch(0, 0, slices // 2), fetch(1, slices // 2, slices)
    for copy in fetches:
        copy.start()
    mask_copy = pltpu.make_async_copy(mask_hbm, mask_own, mask_sem)
    mask_copy.start()
    band_copy = pltpu.make_async_copy(band_hbm, bandv, band_sem)
    band_copy.start()
    taper_copy = pltpu.make_async_copy(taper_hbm, taper_ref, taper_sem)
    taper_copy.start()

    before, after = beside(RCV, -1), beside(RCV, 1)
    lower, upper = beside(SRC, -1), beside(SRC, 1)
    has_before, has_after = place(RCV) > 0, place(RCV) < count_of(RCV) - 1
    has_lower, has_upper = place(SRC) > 0, place(SRC) < count_of(SRC) - 1
    near_count, far_count = count_of(NEAR), count_of(FAR)
    near_me, far_me = place(NEAR), place(FAR)
    lines = lax.axis_size("rcv_0")
    direct = slices - RELAYED if lines > 1 else slices
    at_start, at_end = near_me == 0, near_me == near_count - 1
    relays_left = jnp.logical_and(at_start, jnp.logical_not(has_before))
    relays_right = jnp.logical_and(at_end, jnp.logical_not(has_after))
    next_line = {"rcv_0": 1 - lax.axis_index("rcv_0")}

    def tell(semaphore, device):
        pl.semaphore_signal(semaphore, inc=1, device_id=device, device_id_type=MESH)

    barrier = pltpu.get_barrier_semaphore()
    greeted = sum(flag.astype(jnp.int32) for flag in (has_before, has_after, has_lower, has_upper))
    pl.when(has_lower)(lambda: tell(barrier, lower))
    pl.when(has_upper)(lambda: tell(barrier, upper))
    pl.when(has_before)(lambda: tell(barrier, before))
    pl.when(has_after)(lambda: tell(barrier, after))
    for ring in RINGS:
        if count_of(ring) > 1:
            tell(barrier, beside(ring, -1))
            tell(barrier, beside(ring, 1))
            greeted += 2

    if lines > 1:
        pl.when(at_start)(lambda: tell(barrier, beside(NEAR, -1)))
        pl.when(at_end)(lambda: tell(barrier, beside(NEAR, 1)))
        greeted += at_start.astype(jnp.int32) + at_end.astype(jnp.int32)

    def spread_word(turn):
        for ring in RINGS[:3]:
            if count_of(ring) > 1:
                step = 2 if turn and ring == RINGS[2] and count_of(ring) > 4 else 1
                tell(known.at[turn], beside(ring, -step))
                tell(known.at[turn], beside(ring, step))

    def hear_word(turn):
        pl.semaphore_wait(known.at[turn], 2 * sum(count_of(ring) > 1 for ring in RINGS[:3]))

    def to_left(f, device):
        return pltpu.make_async_remote_copy(
            src_ref=xv.at[:, f, pl.ds(0, HALO)], dst_ref=right.at[f],
            send_sem=send_sem.at[0], recv_sem=right_sem.at[f],
            device_id=device, device_id_type=MESH)

    def to_right(f, device):
        return pltpu.make_async_remote_copy(
            src_ref=xv.at[:, f, pl.ds(ROWS - HALO, HALO)], dst_ref=left.at[f],
            send_sem=send_sem.at[1], recv_sem=left_sem.at[f],
            device_id=device, device_id_type=MESH)

    def to_relay(f, rows, buffer, sems, side):
        return pltpu.make_async_remote_copy(
            src_ref=xv.at[:, f, rows], dst_ref=buffer.at[f], send_sem=send_sem.at[side], recv_sem=sems.at[f],
            device_id=next_line, device_id_type=MESH)

    def from_relay(f, source, target, sems, step):
        return pltpu.make_async_remote_copy(
            src_ref=source.at[f], dst_ref=target.at[f], send_sem=send_sem.at[2], recv_sem=sems.at[f],
            device_id=beside(NEAR, step), device_id_type=MESH)

    def aux(i, source, target, device):
        return pltpu.make_async_remote_copy(
            src_ref=source, dst_ref=target, send_sem=aux_send.at[i], recv_sem=aux_recv.at[i],
            device_id=device, device_id_type=MESH)

    masks = ((aux(0, mask_own, mask_right, before), has_before, has_after),
             (aux(1, mask_own, mask_left, after), has_after, has_before))
    ends = ((aux(2, edges, edges_right, lower), has_lower, has_upper),
            (aux(3, edges, edges_left, upper), has_upper, has_lower))
    rims = ((aux(4, rim.at[pl.ds(0, HALO)], rim_right, before), has_before, has_after),
            (aux(5, rim.at[pl.ds(ROWS - HALO, HALO)], rim_left, after), has_after, has_before))

    def start(entries):
        for copy, sends, _ in entries:
            pl.when(sends)(copy.start)

    def arrive(entries):
        for copy, _, receives in entries:
            pl.when(receives)(copy.wait_recv)

    early_left, last_left = jnp.where(at_start, EARLY_FAR, EARLY), jnp.where(at_start, direct, slices)
    early_right, last_right = jnp.where(at_end, EARLY_FAR, EARLY), jnp.where(at_end, direct, slices)

    def bulk(copy, flag, device, first, last):
        @pl.when(flag)
        def _():
            @pl.loop(first, last)
            def _(f):
                copy(f, device).start()

    for copy in (*fetches, mask_copy, taper_copy):
        copy.wait()
    weights = [taper_ref[i] for i in range(5)]
    shift = shift_ref[0]

    with jax.named_scope("pack"):
        def pack(f, packed):
            for c in range(2):
                x0, x1 = xv[c, f, :, :LANES], xv[c, f, :, LANES:]
                lane = lanes_of(x0.shape)
                tips = jnp.where(lane < 2, x0, jnp.where(lane >= LANES - 2, x1, 0.0))
                packed = packed + pltpu.roll(tips, 4 * (c * slices + f) + 2, 1)
            return packed

        edges[...] = lax.fori_loop(0, slices, pack, jnp.zeros(edges.shape, jnp.float32), unroll=4)

    with jax.named_scope("barrier"):
        pl.semaphore_wait(barrier, greeted)
    start(ends)
    start(masks)
    bulk(to_left, has_before, before, 0, early_left)
    bulk(to_right, has_after, after, 0, early_right)
    if lines > 1:
        for flag, rows, buffer, sems, side in (
                (jnp.logical_and(at_start, has_before), pl.ds(0, HALO), left, left_sem, 0),
                (jnp.logical_and(at_end, has_after), pl.ds(ROWS - HALO, HALO), right, right_sem, 1)):
            @pl.when(flag)
            def _():
                @pl.loop(direct, slices)
                def _(f):
                    to_relay(f, rows, buffer, sems, side).start()
    spread_word(0)

    with jax.named_scope("clear"):
        @pl.when(jnp.logical_not(has_before))
        def _():
            mask_left[...] = jnp.zeros_like(mask_left)
            rim_left[...] = jnp.zeros_like(rim_left)
            left[pl.ds(0, direct)] = jnp.zeros((direct, *left.shape[1:]), jnp.float32)

        @pl.when(jnp.logical_not(has_after))
        def _():
            mask_right[...] = jnp.zeros_like(mask_right)
            rim_right[...] = jnp.zeros_like(rim_right)
            right[pl.ds(0, direct)] = jnp.zeros((direct, *right.shape[1:]), jnp.float32)

        @pl.when(jnp.logical_not(has_lower))
        def _():
            edges_left[...] = jnp.zeros_like(edges_left)

        @pl.when(jnp.logical_not(has_upper))
        def _():
            edges_right[...] = jnp.zeros_like(edges_right)

    def put(f, c, first, values):
        for side, value in enumerate(values):
            h, l = halves(value)
            columns = slice(side * LANES, (side + 1) * LANES)
            high[f, pl.ds(c * LANES + first, ROWS), columns] = h
            low[f, pl.ds(c * LANES + first, ROWS), columns] = l

    with jax.named_scope("own"):
        @pl.loop(0, slices, unroll=2)
        def _(f):
            squares = jnp.zeros((1, LANES), jnp.float32)
            for c in range(2):
                x0, x1 = xv[c, f, :, :LANES], xv[c, f, :, LANES:]
                put(f, c, 0, (x0, x1))
                squares += jnp.sum(x0 * x0 + x1 * x1, axis=0, keepdims=True)
            parts[pl.ds(f, 1), :] = squares

    with jax.named_scope("word0"):
        hear_word(0)
        spread_word(1)
    with jax.named_scope("maskwait"):
        arrive(masks)
    lane_half = lanes_of((1, ROWS))
    m_own, m_left, m_right = (m[...].astype(jnp.float32) for m in (mask_own, mask_left, mask_right))
    mask = jnp.concatenate([m_own, jnp.where(lane_half <= 30 + shift, m_right, m_left)], axis=1)

    band_copy.wait()

    with jax.named_scope("bands"):
        @pl.loop(0, slices // 2)
        def _(g):
            lane = lanes_of((ROWS, LANES))
            for odd in range(2):
                f = 2 * g + odd
                pieces = []
                for c in range(2):
                    tile = bandv[c, :, pl.ds(pl.multiple_of(g * LANES, LANES), LANES)]
                    tile = jnp.where((lane >= APER) if odd else (lane < APER), tile, 0.0)
                    turn = shift + (LANES - APER // 2 - odd * APER)
                    tile = pltpu.roll(pltpu.roll(tile, turn, 1), 0, 1, stride=1, stride_axis=0)
                    pieces.append(halves(tile * mask))
                for k in range(2):
                    real, imag = pieces[0][k], pieces[1][k]
                    base = 2 * ROWS * k
                    bands[f, base:base + ROWS, :LANES] = real
                    bands[f, base:base + ROWS, LANES:] = -imag
                    bands[f, base + ROWS:base + 2 * ROWS, :LANES] = imag
                    bands[f, base + ROWS:base + 2 * ROWS, LANES:] = real

    with jax.named_scope("word1"):
        hear_word(1)
        spread_word(2)
    with jax.named_scope("edgewait"):
        arrive(ends)
    rim[...] = jnp.where(lax.rem(lanes_of(rim.shape), 4) < 2, edges_left[...], edges_right[...])
    start(rims)
    bulk(to_left, has_before, before, early_left, last_left)
    bulk(to_right, has_after, after, early_right, last_right)

    with jax.named_scope("word2"):
        hear_word(2)
    with jax.named_scope("rimwait"):
        arrive(rims)

    def blend(r, l):
        rows = rows_of((32, r.shape[1])) + 16
        return jnp.concatenate([r[:16], jnp.where(rows <= 30 + shift, r[16:], l[:32]), l[32:]], axis=0)

    if lines > 1:
        with jax.named_scope("relay"):
            for flag, source, came, target, sems, step in (
                    (relays_left, left, left_sem, right, right_sem, -1),
                    (relays_right, right, right_sem, left, left_sem, 1)):
                @pl.when(flag)
                def _():
                    @pl.loop(direct, slices)
                    def _(f):
                        from_relay(f, source, source, came, step).wait_recv()
                        from_relay(f, source, target, sems, step).start()

    tips = jnp.concatenate([rim[...], blend(rim_right[...], rim_left[...])], axis=0)
    tips_high[...], tips_low[...] = halves(jnp.concatenate([tips, pltpu.roll(tips, LANES // 2, 1)], axis=0))

    def product(f, x_high, x_low):
        wide = jnp.dot(bands[f], x_high, preferred_element_type=jnp.float32)
        thin = jnp.dot(bands[f, :LANES], x_low, preferred_element_type=jnp.float32)
        return wide[:LANES] + wide[LANES:] + thin

    with jax.named_scope("fringe"):
        @pl.loop(0, slices, unroll=2)
        def _(f):
            fringe[f] = pltpu.roll(product(f, tips_high[...], tips_low[...]), LANES - 2 - 4 * f, 1)

    def arrived(f):
        with jax.named_scope("bulkwait"):
            pl.when(has_after)(to_left(f, before).wait_recv)
            pl.when(has_before)(to_right(f, after).wait_recv)

    def finish(f):
        for c in range(2):
            x = blend(right[f, c], left[f, c])
            put(f, c, ROWS, (x[:, :LANES], x[:, LANES:]))
        predicted = product(f, high[f], low[f])
        squares = jnp.zeros((1, LANES), jnp.float32)
        for side, value in enumerate(taper(fringe[f], predicted[:, :LANES], predicted[:, LANES:], weights)):
            columns = slice(side * LANES, (side + 1) * LANES)
            mult_ref[0, f, :, columns] = value[:ROWS]
            mult_ref[1, f, :, columns] = value[ROWS:]
            squares += jnp.sum(value * value, axis=0, keepdims=True)
        parts[pl.ds(slices + f, 1), :] = squares

    @pl.loop(0, slices // 2 - 1)
    def _(g):
        for f in (2 * g, 2 * g + 1):
            arrived(f)
        for f in (2 * g, 2 * g + 1):
            finish(f)

    @pl.loop(slices - 2, slices)
    def _(f):
        arrived(f)
        finish(f)

    shape = parts.shape
    diagonal = lanes_of(shape) == rows_of(shape)

    def to_row(column):
        return jnp.sum(jnp.where(diagonal, column, 0.0), axis=0, keepdims=True)

    def total(rings, me, count, slots, sems, energy, stage, between):
        row[stage] = energy
        slots[me] = energy

        for device in others_of(rings):
            pltpu.make_async_remote_copy(
                src_ref=row.at[stage], dst_ref=slots.at[me], send_sem=sems.at[0], recv_sem=sems.at[1],
                device_id=device, device_id_type=MESH).start()

        between()
        others = slots.at[pl.ds(0, count - 1)]
        every = pltpu.make_async_remote_copy(
            src_ref=others, dst_ref=others, send_sem=sems.at[0], recv_sem=sems.at[1],
            device_id=beside(rings[0], 1), device_id_type=MESH)
        every.wait_recv()
        result = slots[0]
        for slot in range(1, count):
            result = result + slots[slot]
        return result, every

    def sent():
        for copy, sends, _ in masks + ends + rims:
            pl.when(sends)(copy.wait_send)
        for side, flag, device in ((0, has_before, before), (1, has_after, after)):
            @pl.when(flag)
            def _():
                whole = xv.at[:, :, pl.ds(side * (ROWS - HALO), HALO)]
                pltpu.make_async_remote_copy(
                    src_ref=whole, dst_ref=whole, send_sem=send_sem.at[side], recv_sem=send_sem.at[side],
                    device_id=device, device_id_type=MESH).wait_send()

        if lines > 1:
            for flag, buffer in ((relays_left, left), (relays_right, right)):
                @pl.when(flag)
                def _():
                    whole = buffer.at[pl.ds(direct, RELAYED)]
                    pltpu.make_async_remote_copy(
                        src_ref=whole, dst_ref=whole, send_sem=send_sem.at[2], recv_sem=send_sem.at[2],
                        device_id=next_line, device_id_type=MESH).wait_send()

    energy = to_row(jnp.sum(parts[...], axis=1, keepdims=True))
    with jax.named_scope("near"):
        energy, near_all = total(RINGS[2:], near_me, near_count, near, near_sem, energy, 0, sent)
    with jax.named_scope("far"):
        energy, far_all = total(RINGS[:2], far_me, far_count, far, far_sem, energy, 1, near_all.wait_send)
    predicted = pltpu.roll(energy, LANES - slices, 1)
    gain = jnp.sqrt((energy + 1e-06) / (predicted + 1e-06))
    spread = jnp.sum(jnp.where(diagonal[:slices], gain, 0.0), axis=1, keepdims=True)
    gain_ref[...] = jnp.broadcast_to(spread, gain_ref.shape)

    with jax.named_scope("sendwait"):
        far_all.wait_send()


def subtract(x_ref, mult_ref, gain_ref, mult_hbm, prim_hbm, prim, mult_sem, prim_sem):
    slices = prim.shape[1]
    per_group = slices // GROUPS

    def copy(source, target, sem, g):
        part = pl.ds(g * per_group, per_group)
        return pltpu.make_async_copy(source.at[:, part], target.at[:, part], sem.at[g])

    for g in range(GROUPS):
        copy(mult_ref, mult_hbm, mult_sem, g).start()
    for g in range(GROUPS):
        @pl.loop(g * per_group, (g + 1) * per_group)
        def _(f):
            scale = gain_ref[pl.ds(f, 1), :]
            for side in range(2):
                columns = slice(side * LANES, (side + 1) * LANES)
                for c in range(2):
                    prim[c, f, :, columns] = x_ref[c, f, :, columns] - scale * mult_ref[c, f, :, columns]

        copy(prim, prim_hbm, prim_sem, g).start()
    for g in range(GROUPS):
        copy(mult_ref, mult_hbm, mult_sem, g).wait()
        copy(prim, prim_hbm, prim_sem, g).wait()


def per_device(wavefield, surface_band, band_shift, trace_mask, shot_taper):
    _, slices, receivers, shots = wavefield.shape
    near_count, far_count = count_of(NEAR), count_of(FAR)
    hbm = pl.BlockSpec(memory_space=pltpu.HBM)
    scalars = pl.BlockSpec(memory_space=pltpu.SMEM)
    whole = pl.BlockSpec(memory_space=pltpu.VMEM)
    f32, bf16 = jnp.float32, jnp.bfloat16
    dma = pltpu.SemaphoreType.DMA
    field = jax.ShapeDtypeStruct(wavefield.shape, f32)
    wavefield, surface_band, trace_mask, shot_taper = (
        pltpu.with_memory_space_constraint(a, pltpu.HBM)
        for a in (wavefield, surface_band, trace_mask.reshape(1, receivers), shot_taper))
    held, multiples, gain = pl.pallas_call(
        predict,
        out_shape=(field, field, jax.ShapeDtypeStruct((slices, LANES), f32)),
        in_specs=[hbm, hbm, scalars, hbm, hbm],
        out_specs=(whole, whole, whole),
        scratch_shapes=[
            pltpu.SMEM(shot_taper.shape, f32),
            pltpu.VMEM(surface_band.shape, f32),
            pltpu.VMEM((1, receivers), jnp.int32),
            pltpu.VMEM((1, receivers), jnp.int32),
            pltpu.VMEM((1, receivers), jnp.int32),
            pltpu.VMEM((receivers, LANES), f32),
            pltpu.VMEM((receivers, LANES), f32),
            pltpu.VMEM((receivers, LANES), f32),
            pltpu.VMEM((receivers, LANES), f32),
            pltpu.VMEM((HALO, LANES), f32),
            pltpu.VMEM((HALO, LANES), f32),
            pltpu.VMEM((slices, 2, HALO, shots), f32),
            pltpu.VMEM((slices, 2, HALO, shots), f32),
            pltpu.VMEM((slices, 4 * receivers, 2 * LANES), bf16),
            pltpu.VMEM((slices, 2 * LANES, shots), bf16),
            pltpu.VMEM((slices, 2 * LANES, shots), bf16),
            pltpu.VMEM((4 * receivers, LANES), bf16),
            pltpu.VMEM((4 * receivers, LANES), bf16),
            pltpu.VMEM((slices, 2 * receivers, LANES), f32),
            pltpu.VMEM((2 * slices, LANES), f32),
            pltpu.VMEM((2, 1, LANES), f32),
            pltpu.VMEM((near_count, 1, LANES), f32),
            pltpu.VMEM((far_count, 1, LANES), f32),
            dma((2,)),
            dma(()),
            dma(()),
            dma(()),
            dma((3,)),
            dma((slices,)),
            dma((slices,)),
            dma((6,)),
            dma((6,)),
            dma((2,)),
            dma((2,)),
            pltpu.SemaphoreType.REGULAR((3,)),
        ],
        compiler_params=pltpu.CompilerParams(
            collective_id=0, has_side_effects=True, vmem_limit_bytes=40 * 1024 * 1024),
        name="predict",
    )(wavefield, surface_band, band_shift, trace_mask, shot_taper)
    return pl.pallas_call(
        subtract,
        out_shape=(field, field),
        in_specs=[whole, whole, whole],
        out_specs=(hbm, hbm),
        scratch_shapes=[pltpu.VMEM(wavefield.shape, f32), dma((GROUPS,)), dma((GROUPS,))],
        compiler_params=pltpu.CompilerParams(vmem_limit_bytes=16 * 1024 * 1024),
        name="subtract",
    )(held, multiples, gain)


def solution(mesh):
    split = Mesh(mesh.devices.reshape(SPLIT_SIZES), SRC + RCV)
    return jax.shard_map(
        per_device,
        mesh=split,
        in_specs=(P(None, None, RCV, SRC), P(None, RCV, None), P(RCV), P(RCV), P()),
        out_specs=(P(None, None, RCV, SRC), P(None, None, RCV, SRC)),
        check_vma=False,
    )
```
